512 devices in a mesh: lat: 64 (over y, z), ma: 8 (over x, core).
Axes of the slice: x: 4, y: 8, z: 8, core: 2. Of those that a mesh axis runs over, the one named last changes fastest.
Arguments:
- pair_wave: int32 [360], replicated, may hold values from 0 to 359, each once
- legendre: bfloat16 [360, 640, 768], P('ma', 'lat'), may hold values from -0.0078125 to 0.0078125
- coefs: bfloat16 [360, 768, 168], P('ma', 'lat'), may hold values from -6 to 6
Outputs:
- noise: float32 [53760, 1440], P(('lat', 'ma'))
The draws below stay inside these ranges and needn't reach their ends.
Inputs may be any that keep to these rules, and one draw needn't show every extreme that they name: Slot q holds wavenumbers pair_wave[q] and 719 - pair_wave[q]; every value appears once.
All inputs are finite; a program needn't handle non-finite values.
Results may differ from the reference program's by a relative error of at most 0.0003.
Values may be sent and summed in bfloat16 or wider, within the bound.
No kernel may reach another device: no remote copies, remote signals or barrier semaphores. Data moves between devices by JAX's collectives and lax.ppermute only.
A program may use at most 64 MiB of HBM per device.

```python
import math
import jax
import jax.numpy as jnp
from jax import lax

DEG = 720
LON = 1440
CH = 84
LAT_DEV = 10
PAIRS = 360
RROWS = 768
COLS = 168
LATS = 640
N_LAT = 64
N_MA = 8


def level_of(key, dims, split, smallest, high):
    factor_of = 1.0
    for axis_at, shards_of in split:
        draws = jax.random.uniform(jax.random.fold_in(jax.random.fold_in(key, 6), axis_at), (shards_of,), jnp.float32, smallest / len(split), high / len(split))
        factor_of = factor_of * jnp.repeat(jnp.exp(draws), dims[axis_at] // shards_of).reshape((-1,) + (1,) * (len(dims) - 1 - axis_at))
    return factor_of


def noise(stream_key, extent, deviation, most, shards=(), kind=jnp.bfloat16):
    values = jax.random.normal(stream_key, extent, jnp.float32) * deviation
    if len(shards) > 0:
        values = level_of(stream_key, extent, shards, -0.22, 0.18) * values
    return jnp.clip(values, min=-most, max=most).astype(kind)


def setup_inputs(seed: int = 0) -> dict:
    key_list = jax.random.split(jax.random.key(seed), 4)
    pair_wave = jax.random.permutation(key_list[0], PAIRS).astype(jnp.int32)
    legendre = noise(key_list[1], (PAIRS, LATS, RROWS), (RROWS * DEG) ** -0.5, 0.0078125, ((0, 8), (1, 64)))
    coefs = noise(key_list[2], (PAIRS, RROWS, COLS), 1.0, 6.0, ((0, 8), (1, 64)))
    return dict(pair_wave=pair_wave, legendre=legendre, coefs=coefs)


def chain_table(table, wave_ids, degree_top):
    row_count = table.shape[2]
    row_ids = jnp.arange(row_count, dtype=jnp.int32)[None, :]
    split_row = (degree_top - wave_ids).astype(jnp.int32)[:, None]
    inside = row_ids < split_row
    outside = (row_ids >= split_row) & (row_ids <= degree_top)
    masks = jnp.stack([inside, outside], axis=1)
    return jnp.where(masks[:, :, None, :], table[:, None, :, :], jnp.zeros((), table.dtype))


def fourier_basis(pair_wave, degree_top, lon_count):
    orders = jnp.stack([pair_wave, degree_top - 1 - pair_wave], axis=1).astype(jnp.int32)
    positions = jnp.arange(lon_count, dtype=jnp.int32)
    phase_int = (orders[:, :, None] * positions[None, None, :]) % lon_count
    radians = (2.0 * math.pi / lon_count) * phase_int.astype(jnp.float32)
    weight = jnp.where(orders == 0, 1.0, 2.0).astype(jnp.float32)[:, :, None]
    real_row = weight * jnp.cos(radians)
    imag_row = -weight * jnp.sin(radians)
    return jnp.stack([real_row, imag_row], axis=2).reshape(-1, lon_count)


def reference(pair_wave, legendre, coefs):
    pair_count = pair_wave.shape[0]
    row_count = coefs.shape[1]
    lat_total = LAT_DEV * N_LAT
    slot_count = pair_count // N_MA

    def group_spectra(packed):
        wave_ids, group_table, group_coefs = packed
        masked = chain_table(group_table, wave_ids, DEG)
        return jnp.einsum('qeir,qrc->qeic', masked.astype(jnp.float32), group_coefs.astype(jnp.float32), precision=lax.Precision.HIGHEST)

    spectra = lax.map(group_spectra, (pair_wave.reshape(N_MA, slot_count), legendre.reshape(N_MA, slot_count, lat_total, row_count), coefs.reshape(N_MA, slot_count, row_count, coefs.shape[2])))
    spectra = spectra.reshape(pair_count, 2, lat_total, 2, CH)
    fourier_rows = jnp.transpose(spectra, (0, 1, 3, 2, 4)).reshape(4 * pair_count, lat_total * CH)
    synth_basis = fourier_basis(pair_wave, DEG, LON)
    return lax.dot_general(fourier_rows, synth_basis, (((0,), (0,)), ((), ())), precision=lax.Precision.HIGHEST)
```

```python
import math

import jax
import jax.numpy as jnp
from jax import lax
from jax.sharding import Mesh
from jax.sharding import PartitionSpec as P

DEG = 720
LON = 1440
HALF = LON // 2
CH = 84
LAT_DEV = 10
N_MA = 8
PART = LAT_DEV * CH // N_MA
LANES = 128
LAT = ("y", "z")
MA = ("x", "core")
ALL = ("y", "z", "x", "core")
TOP = 14


def packed(legendre, coefs):
    slots = legendre.shape[0]
    weights = legendre.reshape(slots, -1, LANES)
    main = coefs[:, :, :LANES]
    rest = coefs[:, :, LANES:]
    rest = jnp.transpose(rest.reshape(slots, 3, 4, -1), (0, 2, 1, 3)).reshape(slots, 4, -1)
    rest = jnp.pad(rest, ((0, 0), (0, 0), (0, LANES - rest.shape[2])))
    return jnp.concatenate([weights, main, rest], axis=1)


def unpacked(rows, lat_rows, coef_rows, columns):
    devices = rows.shape[0]
    at = lat_rows * 6
    weights = rows[:, :at].reshape(devices * lat_rows, 6 * LANES)
    main = rows[:, at : at + coef_rows]
    width = columns - LANES
    rest = rows[:, at + coef_rows :, : 3 * width].reshape(devices, 4, 3, width)
    rest = jnp.transpose(rest, (0, 2, 1, 3)).reshape(devices, coef_rows, width)
    coefs = jnp.concatenate([main, rest], axis=2).reshape(devices * coef_rows, columns)
    return weights, coefs


def in_two(full):
    high = lax.reduce_precision(full, 8, 7)
    return high.astype(jnp.bfloat16), (full - high).astype(jnp.bfloat16)


def basis(pair_wave, slots):
    first = pair_wave.reshape(N_MA, slots).T.reshape(-1)
    other = DEG - 1 - first
    is_even = first % 2 == 0
    waves = jnp.stack([jnp.where(is_even, first, other), jnp.where(is_even, other, first)])
    positions = jnp.arange(HALF, dtype=jnp.int32)
    phase = waves[:, :, None] * positions[None, None, :] % LON
    radians = 2.0 * math.pi / LON * phase.astype(jnp.float32)
    weight = jnp.where(waves == 0, 1.0, 2.0).astype(jnp.float32)[:, :, None]
    full = jnp.stack([weight * jnp.cos(radians), -weight * jnp.sin(radians)], axis=1)
    return in_two(full)


def body(pair_wave, legendre, coefs):
    lat_count = lax.axis_size(LAT)
    lat_place = lax.axis_index(LAT)
    ma_place = lax.axis_index(MA)
    slots, lat_rows, degree_rows = legendre.shape
    coef_rows, columns = coefs.shape[1:]
    sent = packed(legendre, coefs)
    sent = jnp.pad(sent, ((0, lat_count - slots), (0, 0), (0, 0)))
    sent = sent.reshape(lat_count, -1, 4, LANES)
    got = lax.all_to_all(sent, LAT, split_axis=0, concat_axis=0, tiled=True)
    weights, packed_coefs = unpacked(
        got.reshape(lat_count, -1, LANES), lat_rows, coef_rows, columns
    )
    slot = ma_place * slots + jnp.minimum(lat_place, slots - 1)
    wave = lax.dynamic_index_in_dim(pair_wave, slot, keepdims=False)
    row_ids = jnp.arange(degree_rows, dtype=jnp.int32)[:, None]
    inside = row_ids < DEG - wave
    outside = (row_ids >= DEG - wave) & (row_ids <= DEG)
    is_even = wave % 2 == 0
    zero = jnp.zeros((), coefs.dtype)
    even = jnp.where(jnp.where(is_even, inside, outside), packed_coefs, zero)
    odd = jnp.where(jnp.where(is_even, outside, inside), packed_coefs, zero)
    sums = jnp.dot(
        weights, jnp.concatenate([even, odd], axis=1), preferred_element_type=jnp.float32
    )
    largest = jnp.max(jnp.abs(sums))
    power = jnp.clip(jnp.floor(jnp.log2(jnp.maximum(largest, 1e-30))), -100.0, 100.0)
    parts = jnp.transpose(sums.reshape(lat_count, lat_rows, 4, CH), (0, 2, 1, 3))
    parts = parts.reshape(lat_count, 4, N_MA, PART) * jnp.exp2(TOP - power)
    parts = jnp.transpose(parts, (0, 2, 1, 3)).reshape(lat_count * N_MA, 4, PART)
    note = jnp.broadcast_to(power, (lat_count * N_MA, 4, LANES - PART))
    parts = jnp.concatenate([parts, note], axis=2).astype(jnp.float16)
    spectra = lax.all_to_all(parts, ALL, split_axis=0, concat_axis=0, tiled=True)
    spectra = spectra[: slots * N_MA].astype(jnp.float32)
    spectra = spectra * jnp.exp2(spectra[:, :, PART:][:, :, :1] - TOP)
    spectra = spectra[:, :, :PART]
    high, low = in_two(spectra)
    base_high, base_low = basis(pair_wave, slots)

    def times(h, b, parity):
        return lax.dot_general(
            h[:, 2 * parity : 2 * parity + 2],
            b[parity],
            (((1, 0), (0, 1)), ((), ())),
            preferred_element_type=jnp.float32,
        )

    halves = [
        times(high, base_high, k) + times(low, base_high, k) + times(high, base_low, k)
        for k in range(2)
    ]
    return jnp.concatenate([halves[0] + halves[1], halves[0] - halves[1]], axis=1)


def solution(mesh):
    split = Mesh(mesh.devices.reshape(8, mesh.shape["lat"] // 8, 4, 2), ALL)
    placed = (P(), P(MA, LAT, None), P(MA, LAT, None))
    return jax.shard_map(
        body, mesh=split, in_specs=placed, out_specs=P(ALL, None), check_vma=False
    )
```

```python
import functools
import math

import jax
import jax.numpy as jnp
from jax import lax
from jax.experimental import pallas as pl
from jax.experimental.pallas import tpu as pltpu
from jax.sharding import Mesh
from jax.sharding import PartitionSpec as P

DEG = 720
LON = 1440
HALF = LON // 2
CH = 84
LAT_DEV = 10
N_MA = 8
PART = LAT_DEV * CH // N_MA
LANES = 128
LAT = ("y", "z")
MA = ("x", "core")
ALL = ("y", "z", "x", "core")
TOP = 14


def sums_kernel(wave_ref, got_ref, out_ref, wide_ref, weights_ref, real_ref, imag_ref, sums_ref, turned_ref, *, lat_count, lat_rows, coef_rows):
    chunk = got_ref.shape[0] // lat_count
    blocks = DEG // LANES + 1
    depth = lat_count * coef_rows
    wide_ref[...] = got_ref[...].astype(jnp.float32)
    for i in range(lat_rows):
        for b in range(blocks):
            piece = wide_ref[pl.ds(i * blocks + b, lat_count, stride=chunk), :]
            weights_ref[i * lat_count : (i + 1) * lat_count, b * LANES : (b + 1) * LANES] = piece.astype(jnp.bfloat16)
    at = lat_rows * blocks
    tail = 2 * CH - LANES
    lane = lax.broadcasted_iota(jnp.int32, (lat_count, LANES), 1)
    for k in range(coef_rows):
        main = wide_ref[pl.ds(at + k, lat_count, stride=chunk), :]
        rest = wide_ref[pl.ds(at + coef_rows + k % 4, lat_count, stride=chunk), :]
        split = LANES - CH
        moved = pltpu.roll(main, LANES - CH, 1)
        rest = pltpu.roll(rest, (split - tail * (k // 4)) % LANES, 1)
        imag = jnp.where(lane < split, moved, rest)
        real_ref[pl.ds(k, lat_count, stride=coef_rows), :] = jnp.where(lane < CH, main, 0.0)
        imag_ref[pl.ds(k, lat_count, stride=coef_rows), :] = jnp.where(lane < CH, imag, 0.0)
    wave = wave_ref[0]
    row = lax.broadcasted_iota(jnp.int32, (depth, 2 * LANES), 0)
    inside = row < DEG - wave
    outside = jnp.logical_and(row >= DEG - wave, row <= DEG)
    both = jnp.concatenate([real_ref[...], imag_ref[...]], axis=1)
    is_even = wave % 2 == 0
    first = jnp.where(inside, both, 0.0)
    second = jnp.where(outside, both, 0.0)
    even = jnp.where(is_even, first, second).astype(jnp.bfloat16)
    odd = jnp.where(is_even, second, first).astype(jnp.bfloat16)
    weights = weights_ref[...]
    even = jnp.dot(weights, even, preferred_element_type=jnp.float32)
    odd = jnp.dot(weights, odd, preferred_element_type=jnp.float32)
    sums_ref[:, : 2 * LANES] = even
    sums_ref[:, 2 * LANES :] = odd
    largest = jnp.maximum(jnp.max(jnp.abs(even)), jnp.max(jnp.abs(odd)))
    largest = jnp.maximum(jnp.full((lat_count, LANES), largest, jnp.float32), 1e-30)
    power = jnp.clip(jnp.floor(jnp.log2(largest)), -100.0, 100.0)
    scale = jnp.exp2(TOP - power)
    pitch = turned_ref.shape[0] // lat_count
    for a in range(N_MA):
        i, off = divmod(a * PART, CH)
        for he in range(4):
            cols = slice(he * LANES, (he + 1) * LANES)
            near = sums_ref[i * lat_count : (i + 1) * lat_count, cols]
            far = sums_ref[(i + 1) * lat_count : (i + 2) * lat_count, cols]
            if off:
                near = pltpu.roll(near, LANES - off, 1)
            far = pltpu.roll(far, CH - off, 1)
            value = jnp.where(lane < CH - off, near, far) * scale
            value = jnp.where(lane < PART, value, power)
            turned_ref[pl.ds(a * 4 + he, lat_count, stride=pitch), :] = value
    rows = 4 * N_MA
    for l in range(lat_count):
        out_ref[l * rows : (l + 1) * rows, :] = turned_ref[l * pitch : l * pitch + rows, :]


def sums_call(wave, got, lat_count, lat_rows, coef_rows):
    blocks = DEG // LANES + 1
    vm = pltpu.VMEM
    return pl.pallas_call(
        functools.partial(sums_kernel, lat_count=lat_count, lat_rows=lat_rows, coef_rows=coef_rows),
        out_shape=pltpu.VMEM((lat_count * N_MA * 4, LANES), jnp.float32),
        in_specs=[pl.BlockSpec(memory_space=pltpu.SMEM), pl.BlockSpec(memory_space=vm)],
        out_specs=pl.BlockSpec(memory_space=vm),
        scratch_shapes=[
            vm(got.shape, jnp.float32),
            vm((lat_count * lat_rows, blocks * LANES), jnp.bfloat16),
            vm((lat_count * coef_rows, LANES), jnp.float32),
            vm((lat_count * coef_rows, LANES), jnp.float32),
            vm((lat_count * lat_rows, 4 * LANES), jnp.float32),
            vm((lat_count * (4 * N_MA + 4), LANES), jnp.float32),
        ],
    )(wave, got)


def pack_kernel(legendre_ref, coefs_ref, out_ref, wide_ref):
    lat_rows, slots, degree_rows = legendre_ref.shape
    coef_rows = coefs_ref.shape[0]
    blocks = degree_rows // LANES
    chunk = lat_rows * blocks + coef_rows + 4
    for i in range(lat_rows):
        for b in range(blocks):
            piece = legendre_ref[i, :, b * LANES : (b + 1) * LANES].astype(jnp.float32)
            wide_ref[pl.ds(i * blocks + b, slots, stride=chunk), :] = piece
    at = lat_rows * blocks
    tail = 2 * CH - LANES
    for k in range(coef_rows):
        wide_ref[pl.ds(at + k, slots, stride=chunk), :] = coefs_ref[k, :, :LANES].astype(jnp.float32)
    for t in range(4):
        parts = [coefs_ref[t + 4 * j, :, LANES:].astype(jnp.float32) for j in range(3)]
        parts.append(jnp.zeros((slots, LANES - 3 * tail), jnp.float32))
        wide_ref[pl.ds(at + coef_rows + t, slots, stride=chunk), :] = jnp.concatenate(parts, axis=1)
    full = slots * chunk
    out_ref[:full, :] = wide_ref[...].astype(jnp.bfloat16)
    out_ref[full:, :] = jnp.zeros((out_ref.shape[0] - full, LANES), jnp.bfloat16)


def pack_call(legendre, coefs, lat_count):
    slots, lat_rows, degree_rows = legendre.shape
    coef_rows = coefs.shape[1]
    chunk = lat_rows * degree_rows // LANES + coef_rows + 4
    vm = pltpu.VMEM
    return pl.pallas_call(
        pack_kernel,
        out_shape=jax.ShapeDtypeStruct((lat_count * chunk, LANES), jnp.bfloat16),
        in_specs=[pl.BlockSpec(memory_space=vm)] * 2,
        out_specs=pl.BlockSpec(memory_space=vm),
        scratch_shapes=[vm((slots * chunk, LANES), jnp.float32)],
    )(jnp.transpose(legendre, (1, 0, 2)), jnp.transpose(coefs, (1, 0, 2)))


def in_two(full):
    high = lax.reduce_precision(full, 8, 7)
    return high.astype(jnp.bfloat16), (full - high).astype(jnp.bfloat16)


def basis(pair_wave, slots):
    first = pair_wave.reshape(N_MA, slots).T.reshape(-1)
    other = DEG - 1 - first
    is_even = first % 2 == 0
    waves = jnp.stack([jnp.where(is_even, first, other), jnp.where(is_even, other, first)])
    positions = jnp.arange(HALF, dtype=jnp.int32)
    phase = waves[:, :, None] * positions[None, None, :] % LON
    radians = 2.0 * math.pi / LON * phase.astype(jnp.float32)
    weight = jnp.where(waves == 0, 1.0, 2.0).astype(jnp.float32)[:, :, None]
    full = jnp.stack([weight * jnp.cos(radians), -weight * jnp.sin(radians)], axis=1)
    return in_two(full)


def body(pair_wave, legendre, coefs):
    lat_count = lax.axis_size(LAT)
    lat_place = lax.axis_index(LAT)
    ma_place = lax.axis_index(MA)
    slots, lat_rows = legendre.shape[:2]
    coef_rows = coefs.shape[1]
    sent = pack_call(legendre, coefs, lat_count).reshape(lat_count, -1, 4, LANES)
    got = lax.all_to_all(sent, LAT, split_axis=0, concat_axis=0, tiled=True)
    slot = ma_place * slots + jnp.minimum(lat_place, slots - 1)
    wave = lax.dynamic_slice_in_dim(pair_wave, slot, 1)
    got = pltpu.with_memory_space_constraint(got.reshape(-1, LANES), pltpu.VMEM)
    parts = sums_call(wave, got, lat_count, lat_rows, coef_rows)
    parts = parts.astype(jnp.float16).reshape(lat_count * N_MA, 4, LANES)
    spectra = lax.all_to_all(parts, ALL, split_axis=0, concat_axis=0, tiled=True)
    spectra = spectra[: slots * N_MA].astype(jnp.float32)
    spectra = spectra * jnp.exp2(spectra[:, :, PART:][:, :, :1] - TOP)
    spectra = spectra[:, :, :PART]
    high, low = in_two(spectra)
    base_high, base_low = basis(pair_wave, slots)

    def times(h, b, parity):
        return lax.dot_general(
            h[:, 2 * parity : 2 * parity + 2],
            b[parity],
            (((1, 0), (0, 1)), ((), ())),
            preferred_element_type=jnp.float32,
        )

    halves = [
        times(high, base_high, k) + times(low, base_high, k) + times(high, base_low, k)
        for k in range(2)
    ]
    return jnp.concatenate([halves[0] + halves[1], halves[0] - halves[1]], axis=1)


def solution(mesh):
    split = Mesh(mesh.devices.reshape(8, mesh.shape["lat"] // 8, 4, 2), ALL)
    placed = (P(), P(MA, LAT, None), P(MA, LAT, None))
    return jax.shard_map(
        body, mesh=split, in_specs=placed, out_specs=P(ALL, None), check_vma=False
    )
```

```python
import functools
import math

import jax
import jax.numpy as jnp
from jax import lax
from jax.experimental import pallas as pl
from jax.experimental.pallas import tpu as pltpu
from jax.sharding import Mesh
from jax.sharding import PartitionSpec as P

DEG = 720
LON = 1440
HALF = LON // 2
CH = 84
LAT_DEV = 10
N_MA = 8
PART = LAT_DEV * CH // N_MA
LANES = 128
LAT = ("y", "z")
MA = ("x", "core")
ALL = ("y", "z", "x", "core")
TOP = 14
GRANT = 24 * 2**20
FETCHES = 5


def sums_kernel(wave_ref, got_ref, out_ref, wide_ref, weights_ref, real_ref, imag_ref, sums_ref, turned_ref, *, lat_count, lat_rows, coef_rows):
    chunk = got_ref.shape[0] // lat_count
    blocks = DEG // LANES + 1
    depth = lat_count * coef_rows
    wide_ref[...] = got_ref[...].astype(jnp.float32)
    for i in range(lat_rows):
        for b in range(blocks):
            piece = wide_ref[pl.ds(i * blocks + b, lat_count, stride=chunk), :]
            weights_ref[i * lat_count : (i + 1) * lat_count, b * LANES : (b + 1) * LANES] = piece.astype(jnp.bfloat16)
    at = lat_rows * blocks
    tail = 2 * CH - LANES
    split = LANES - CH
    lane = lax.broadcasted_iota(jnp.int32, (lat_count, LANES), 1)
    for k in range(coef_rows):
        main = wide_ref[pl.ds(at + k, lat_count, stride=chunk), :]
        row, place = tail_place(k, lat_rows, coef_rows, blocks, tail)
        rest = wide_ref[pl.ds(row, lat_count, stride=chunk), :]
        moved = pltpu.roll(main, split, 1)
        rest = pltpu.roll(rest, (split - place) % LANES, 1)
        imag = jnp.where(lane < split, moved, rest)
        real_ref[pl.ds(k, lat_count, stride=coef_rows), :] = jnp.where(lane < CH, main, 0.0)
        imag_ref[pl.ds(k, lat_count, stride=coef_rows), :] = jnp.where(lane < CH, imag, 0.0)
    wave = wave_ref[0]
    row = lax.broadcasted_iota(jnp.int32, (depth, 2 * LANES), 0)
    inside = row < DEG - wave
    outside = jnp.logical_and(row >= DEG - wave, row <= DEG)
    both = jnp.concatenate([real_ref[...], imag_ref[...]], axis=1)
    is_even = wave % 2 == 0
    first = jnp.where(inside, both, 0.0)
    second = jnp.where(outside, both, 0.0)
    even = jnp.where(is_even, first, second).astype(jnp.bfloat16)
    odd = jnp.where(is_even, second, first).astype(jnp.bfloat16)
    weights = weights_ref[...]
    even = jnp.dot(weights, even, preferred_element_type=jnp.float32)
    odd = jnp.dot(weights, odd, preferred_element_type=jnp.float32)
    sums_ref[:, : 2 * LANES] = even
    sums_ref[:, 2 * LANES :] = odd
    largest = jnp.maximum(jnp.max(jnp.abs(even)), jnp.max(jnp.abs(odd)))
    largest = jnp.maximum(jnp.full((lat_count, LANES), largest, jnp.float32), 1e-30)
    power = jnp.clip(jnp.floor(jnp.log2(largest)), -100.0, 100.0)
    scale = jnp.exp2(TOP - power)
    pitch = turned_ref.shape[0] // lat_count
    for a in range(N_MA):
        i, off = divmod(a * PART, CH)
        for he in range(4):
            cols = slice(he * LANES, (he + 1) * LANES)
            near = sums_ref[i * lat_count : (i + 1) * lat_count, cols]
            far = sums_ref[(i + 1) * lat_count : (i + 2) * lat_count, cols]
            if off:
                near = pltpu.roll(near, LANES - off, 1)
            far = pltpu.roll(far, CH - off, 1)
            value = jnp.where(lane < CH - off, near, far) * scale
            value = jnp.where(lane < PART, value, power)
            turned_ref[pl.ds(a * 4 + he, lat_count, stride=pitch), :] = value
    rows = 4 * N_MA
    for l in range(lat_count):
        out_ref[l * rows : (l + 1) * rows, :] = turned_ref[l * pitch : l * pitch + rows, :]


def sums_call(wave, got, lat_count, lat_rows, coef_rows):
    blocks = DEG // LANES + 1
    vm = pltpu.VMEM
    return pl.pallas_call(
        functools.partial(sums_kernel, lat_count=lat_count, lat_rows=lat_rows, coef_rows=coef_rows),
        out_shape=pltpu.VMEM((lat_count * N_MA * 4, LANES), jnp.float32),
        in_specs=[pl.BlockSpec(memory_space=pltpu.SMEM), pl.BlockSpec(memory_space=vm)],
        out_specs=pl.BlockSpec(memory_space=vm),
        scratch_shapes=[
            vm(got.shape, jnp.float32),
            vm((lat_count * lat_rows, blocks * LANES), jnp.bfloat16),
            vm((lat_count * coef_rows, LANES), jnp.float32),
            vm((lat_count * coef_rows, LANES), jnp.float32),
            vm((lat_count * lat_rows, 4 * LANES), jnp.float32),
            vm((lat_count * (4 * N_MA + 4), LANES), jnp.float32),
        ],
        compiler_params=pltpu.CompilerParams(vmem_limit_bytes=GRANT),
    )(wave, got)


def pack_kernel(legendre_ref, coefs_ref, out_ref, wide_ref):
    lat_rows, slots, degree_rows = legendre_ref.shape
    coef_rows = coefs_ref.shape[0]
    blocks = degree_rows // LANES
    chunk = chunk_rows(lat_rows, coef_rows, blocks)
    tail = 2 * CH - LANES
    top = wide_ref.shape[0]
    wide_ref[top - 16 :, :] = jnp.zeros((16, LANES), jnp.float32)
    for i in range(lat_rows):
        for b in range(blocks):
            piece = legendre_ref[i, :, b * LANES : (b + 1) * LANES].astype(jnp.float32)
            if b == blocks - 1:
                rest = coefs_ref[i, :, LANES:].astype(jnp.float32)
                piece = jnp.concatenate([piece[:, : LANES - tail], rest], axis=1)
            wide_ref[pl.ds(i * blocks + b, slots, stride=chunk), :] = piece
    at = lat_rows * blocks
    for k in range(coef_rows):
        piece = coefs_ref[k, :, :LANES].astype(jnp.float32)
        wide_ref[pl.ds(at + k, slots, stride=chunk), :] = piece
    last = [coefs_ref[k, :, LANES:].astype(jnp.float32) for k in range(lat_rows, coef_rows)]
    last.append(jnp.zeros((slots, LANES - len(last) * tail), jnp.float32))
    last = jnp.concatenate(last, axis=1)
    for t in range(at + coef_rows, chunk):
        wide_ref[pl.ds(t, slots, stride=chunk), :] = last
    out_ref[:top, :] = wide_ref[...].astype(jnp.bfloat16)
    out_ref[top:, :] = jnp.zeros((out_ref.shape[0] - top, LANES), jnp.bfloat16)


def chunk_rows(lat_rows, coef_rows, blocks):
    rows = lat_rows * blocks + coef_rows + 1
    return rows + rows % 2


def tail_place(k, lat_rows, coef_rows, blocks, tail):
    if k < lat_rows:
        return k * blocks + blocks - 1, LANES - tail
    return lat_rows * blocks + coef_rows, (k - lat_rows) * tail


def pack_call(legendre, coefs, lat_count):
    slots, lat_rows, degree_rows = legendre.shape
    coef_rows = coefs.shape[1]
    chunk = chunk_rows(lat_rows, coef_rows, degree_rows // LANES)
    vm = pltpu.VMEM
    return pl.pallas_call(
        pack_kernel,
        out_shape=jax.ShapeDtypeStruct((lat_count * chunk, LANES), jnp.bfloat16),
        in_specs=[pl.BlockSpec(memory_space=vm)] * 2,
        out_specs=pl.BlockSpec(memory_space=vm),
        scratch_shapes=[vm((-(-slots * chunk // 16) * 16, LANES), jnp.float32)],
    )(jnp.transpose(legendre, (1, 0, 2)), jnp.transpose(coefs, (1, 0, 2)))


def synth_kernel(spectra_ref, high_ref, low_hbm, out_ref, low_ref, sems):
    step = low_ref.shape[1] // FETCHES
    fetches = []
    for parity in range(2):
        for k in range(FETCHES):
            part = pl.ds(k * step, step)
            fetches.append(
                pltpu.make_async_copy(
                    low_hbm.at[parity, part],
                    low_ref.at[parity, part],
                    sems.at[parity * FETCHES + k],
                )
            )
            fetches[-1].start()
    count = spectra_ref.shape[0] // 4
    over_rows = (((0,), (0,)), ((), ()))
    highs, sums = [], []
    for parity in range(2):
        rows = []
        for e in range(2):
            row = spectra_ref[pl.ds(2 * parity + e, count, stride=4), :]
            rows.append(row * jnp.exp2(row[:, LANES - 1 :] - TOP))
        row = jnp.concatenate(rows, axis=0)
        high = row.astype(jnp.bfloat16)
        low = (row - high.astype(jnp.float32)).astype(jnp.bfloat16)
        both = lax.dot_general(
            jnp.concatenate([high, low], axis=1),
            high_ref[parity],
            over_rows,
            preferred_element_type=jnp.float32,
        )
        highs.append(high)
        sums.append(both[:LANES] + both[LANES:])
    for parity in range(2):
        for k in range(FETCHES):
            fetches[parity * FETCHES + k].wait()
        more = lax.dot_general(
            highs[parity], low_ref[parity], over_rows, preferred_element_type=jnp.float32
        )
        sums[parity] = (sums[parity] + more)[:PART]
    out_ref[:, :HALF] = sums[0] + sums[1]
    out_ref[:, HALF:] = sums[0] - sums[1]


def synth_call(spectra, high, low):
    vm = pltpu.VMEM
    return pl.pallas_call(
        synth_kernel,
        out_shape=jax.ShapeDtypeStruct((PART, LON), jnp.float32),
        in_specs=[pl.BlockSpec(memory_space=vm)] * 2 + [pl.BlockSpec(memory_space=pltpu.HBM)],
        out_specs=pl.BlockSpec(memory_space=vm),
        scratch_shapes=[vm(low.shape, low.dtype), pltpu.SemaphoreType.DMA((2 * FETCHES,))],
        compiler_params=pltpu.CompilerParams(vmem_limit_bytes=GRANT),
    )(spectra, high, low)


def halve_kernel(full_ref, high_ref, low_ref):
    full = full_ref[...]
    high = full.astype(jnp.bfloat16)
    high_ref[...] = high
    low_ref[...] = (full - high.astype(jnp.float32)).astype(jnp.bfloat16)


def halve_call(full):
    parities, rows, columns = full.shape
    block = pl.BlockSpec((None, rows, columns), lambda p: (p, 0, 0))
    return pl.pallas_call(
        halve_kernel,
        grid=(parities,),
        out_shape=[
            pltpu.VMEM(full.shape, jnp.bfloat16),
            pltpu.HBM(full.shape, jnp.bfloat16),
        ],
        in_specs=[block],
        out_specs=[block] * 2,
        compiler_params=pltpu.CompilerParams(vmem_limit_bytes=GRANT),
    )(full)


def basis(pair_wave, slots):
    first = pair_wave.reshape(N_MA, slots).T.reshape(-1)
    other = DEG - 1 - first
    is_even = first % 2 == 0
    waves = jnp.stack([jnp.where(is_even, first, other), jnp.where(is_even, other, first)])
    positions = jnp.arange(HALF, dtype=jnp.int32)
    phase = waves[:, :, None] * positions[None, None, :] % LON
    radians = 2.0 * math.pi / LON * phase.astype(jnp.float32)
    weight = jnp.where(waves == 0, 1.0, 2.0).astype(jnp.float32)[:, :, None]
    full = jnp.stack([weight * jnp.cos(radians), -weight * jnp.sin(radians)], axis=1)
    return full.reshape(2, -1, HALF)


def body(pair_wave, legendre, coefs):
    lat_count = lax.axis_size(LAT)
    lat_place = lax.axis_index(LAT)
    ma_place = lax.axis_index(MA)
    slots, lat_rows = legendre.shape[:2]
    coef_rows = coefs.shape[1]
    sent = pack_call(legendre, coefs, lat_count).reshape(lat_count, -1, 2, LANES)
    got = lax.all_to_all(sent, LAT, split_axis=0, concat_axis=0, tiled=True)
    slot = ma_place * slots + jnp.minimum(lat_place, slots - 1)
    wave = lax.dynamic_slice_in_dim(pair_wave, slot, 1)
    got = pltpu.with_memory_space_constraint(got.reshape(-1, LANES), pltpu.VMEM)
    parts = sums_call(wave, got, lat_count, lat_rows, coef_rows)
    parts = parts.astype(jnp.float16).reshape(lat_count * N_MA, 4, LANES)
    spectra = lax.all_to_all(parts, ALL, split_axis=0, concat_axis=0, tiled=True)
    spectra = spectra[: slots * N_MA].astype(jnp.float32).reshape(-1, LANES)
    high, low = halve_call(basis(pair_wave, slots))
    high = pltpu.with_memory_space_constraint(high, pltpu.VMEM)
    low = pltpu.with_memory_space_constraint(low, pltpu.HBM)
    spectra = pltpu.with_memory_space_constraint(spectra, pltpu.VMEM)
    return synth_call(spectra, high, low)


def solution(mesh):
    split = Mesh(mesh.devices.reshape(8, mesh.shape["lat"] // 8, 4, 2), ALL)
    placed = (P(), P(MA, LAT, None), P(MA, LAT, None))
    return jax.shard_map(
        body, mesh=split, in_specs=placed, out_specs=P(ALL, None), check_vma=False
    )
```

```python
import functools
import math

import jax
import jax.numpy as jnp
from jax import lax
from jax.experimental import pallas as pl
from jax.experimental.pallas import tpu as pltpu
from jax.sharding import Mesh
from jax.sharding import PartitionSpec as P

DEG = 720
LON = 1440
QUARTER = LON // 4
CH = 84
LAT_DEV = 10
N_MA = 8
PART = LAT_DEV * CH // N_MA
LANES = 128
LAT = ("y", "z")
MA = ("x", "core")
ALL = ("y", "z", "x", "core")
TOP = 14
GRANT = 24 * 2**20


def sums_kernel(wave_ref, got_ref, out_ref, wide_ref, weights_ref, real_ref, imag_ref, sums_ref, turned_ref, *, lat_count, lat_rows, coef_rows):
    chunk = got_ref.shape[0] // lat_count
    blocks = DEG // LANES + 1
    depth = lat_count * coef_rows
    wide_ref[...] = got_ref[...].astype(jnp.float32)
    for i in range(lat_rows):
        for b in range(blocks):
            piece = wide_ref[pl.ds(i * blocks + b, lat_count, stride=chunk), :]
            weights_ref[i * lat_count : (i + 1) * lat_count, b * LANES : (b + 1) * LANES] = piece.astype(jnp.bfloat16)
    at = lat_rows * blocks
    tail = 2 * CH - LANES
    split = LANES - CH
    lane = lax.broadcasted_iota(jnp.int32, (lat_count, LANES), 1)
    for k in range(coef_rows):
        main = wide_ref[pl.ds(at + k, lat_count, stride=chunk), :]
        row, place = tail_place(k, lat_rows, coef_rows, blocks, tail)
        rest = wide_ref[pl.ds(row, lat_count, stride=chunk), :]
        moved = pltpu.roll(main, split, 1)
        rest = pltpu.roll(rest, (split - place) % LANES, 1)
        imag = jnp.where(lane < split, moved, rest)
        real_ref[pl.ds(k, lat_count, stride=coef_rows), :] = jnp.where(lane < CH, main, 0.0)
        imag_ref[pl.ds(k, lat_count, stride=coef_rows), :] = jnp.where(lane < CH, imag, 0.0)
    wave = wave_ref[0]
    row = lax.broadcasted_iota(jnp.int32, (depth, 2 * LANES), 0)
    inside = row < DEG - wave
    outside = jnp.logical_and(row >= DEG - wave, row <= DEG)
    both = jnp.concatenate([real_ref[...], imag_ref[...]], axis=1)
    is_even = wave % 2 == 0
    first = jnp.where(inside, both, 0.0)
    second = jnp.where(outside, both, 0.0)
    even = jnp.where(is_even, first, second).astype(jnp.bfloat16)
    odd = jnp.where(is_even, second, first).astype(jnp.bfloat16)
    weights = weights_ref[...]
    even = jnp.dot(weights, even, preferred_element_type=jnp.float32)
    odd = jnp.dot(weights, odd, preferred_element_type=jnp.float32)
    sums_ref[:, : 2 * LANES] = even
    sums_ref[:, 2 * LANES :] = odd
    largest = jnp.maximum(jnp.max(jnp.abs(even)), jnp.max(jnp.abs(odd)))
    largest = jnp.maximum(jnp.full((lat_count, LANES), largest, jnp.float32), 1e-30)
    power = jnp.clip(jnp.floor(jnp.log2(largest)), -100.0, 100.0)
    scale = jnp.exp2(TOP - power)
    pitch = turned_ref.shape[0] // lat_count
    for a in range(N_MA):
        i, off = divmod(a * PART, CH)
        for he in range(4):
            cols = slice(he * LANES, (he + 1) * LANES)
            near = sums_ref[i * lat_count : (i + 1) * lat_count, cols]
            far = sums_ref[(i + 1) * lat_count : (i + 2) * lat_count, cols]
            if off:
                near = pltpu.roll(near, LANES - off, 1)
            far = pltpu.roll(far, CH - off, 1)
            value = jnp.where(lane < CH - off, near, far) * scale
            value = jnp.where(lane < PART, value, power)
            turned_ref[pl.ds(a * 4 + he, lat_count, stride=pitch), :] = value
    rows = 4 * N_MA
    for l in range(lat_count):
        out_ref[l * rows : (l + 1) * rows, :] = turned_ref[l * pitch : l * pitch + rows, :]


def sums_call(wave, got, lat_count, lat_rows, coef_rows):
    blocks = DEG // LANES + 1
    vm = pltpu.VMEM
    return pl.pallas_call(
        functools.partial(sums_kernel, lat_count=lat_count, lat_rows=lat_rows, coef_rows=coef_rows),
        out_shape=pltpu.VMEM((lat_count * N_MA * 4, LANES), jnp.float32),
        in_specs=[pl.BlockSpec(memory_space=pltpu.SMEM), pl.BlockSpec(memory_space=vm)],
        out_specs=pl.BlockSpec(memory_space=vm),
        scratch_shapes=[
            vm(got.shape, jnp.float32),
            vm((lat_count * lat_rows, blocks * LANES), jnp.bfloat16),
            vm((lat_count * coef_rows, LANES), jnp.float32),
            vm((lat_count * coef_rows, LANES), jnp.float32),
            vm((lat_count * lat_rows, 4 * LANES), jnp.float32),
            vm((lat_count * (4 * N_MA + 4), LANES), jnp.float32),
        ],
        compiler_params=pltpu.CompilerParams(vmem_limit_bytes=GRANT),
    )(wave, got)


def pack_kernel(legendre_ref, coefs_ref, out_ref, wide_ref):
    lat_rows, slots, degree_rows = legendre_ref.shape
    coef_rows = coefs_ref.shape[0]
    blocks = degree_rows // LANES
    chunk = chunk_rows(lat_rows, coef_rows, blocks)
    tail = 2 * CH - LANES
    top = wide_ref.shape[0]
    wide_ref[top - 16 :, :] = jnp.zeros((16, LANES), jnp.float32)
    for i in range(lat_rows):
        for b in range(blocks):
            piece = legendre_ref[i, :, b * LANES : (b + 1) * LANES].astype(jnp.float32)
            if b == blocks - 1:
                rest = coefs_ref[i, :, LANES:].astype(jnp.float32)
                piece = jnp.concatenate([piece[:, : LANES - tail], rest], axis=1)
            wide_ref[pl.ds(i * blocks + b, slots, stride=chunk), :] = piece
    at = lat_rows * blocks
    for k in range(coef_rows):
        piece = coefs_ref[k, :, :LANES].astype(jnp.float32)
        wide_ref[pl.ds(at + k, slots, stride=chunk), :] = piece
    last = [coefs_ref[k, :, LANES:].astype(jnp.float32) for k in range(lat_rows, coef_rows)]
    last.append(jnp.zeros((slots, LANES - len(last) * tail), jnp.float32))
    last = jnp.concatenate(last, axis=1)
    for t in range(at + coef_rows, chunk):
        wide_ref[pl.ds(t, slots, stride=chunk), :] = last
    out_ref[:top, :] = wide_ref[...].astype(jnp.bfloat16)
    out_ref[top:, :] = jnp.zeros((out_ref.shape[0] - top, LANES), jnp.bfloat16)


def chunk_rows(lat_rows, coef_rows, blocks):
    rows = lat_rows * blocks + coef_rows + 1
    return rows + rows % 2


def tail_place(k, lat_rows, coef_rows, blocks, tail):
    if k < lat_rows:
        return k * blocks + blocks - 1, LANES - tail
    return lat_rows * blocks + coef_rows, (k - lat_rows) * tail


def pack_call(legendre, coefs, lat_count):
    slots, lat_rows, degree_rows = legendre.shape
    coef_rows = coefs.shape[1]
    chunk = chunk_rows(lat_rows, coef_rows, degree_rows // LANES)
    vm = pltpu.VMEM
    return pl.pallas_call(
        pack_kernel,
        out_shape=jax.ShapeDtypeStruct((lat_count * chunk, LANES), jnp.bfloat16),
        in_specs=[pl.BlockSpec(memory_space=vm)] * 2,
        out_specs=pl.BlockSpec(memory_space=vm),
        scratch_shapes=[vm((-(-slots * chunk // 16) * 16, LANES), jnp.float32)],
    )(jnp.transpose(legendre, (1, 0, 2)), jnp.transpose(coefs, (1, 0, 2)))


def synth_kernel(spectra_ref, signs_ref, basis_ref, out_ref):
    count = spectra_ref.shape[0] // 4
    sums = []
    for parity in range(2):
        sign = signs_ref[parity]
        real, imag = (
            row * jnp.exp2(row[:, LANES - 1 :] - TOP)
            for row in (
                spectra_ref[pl.ds(2 * parity + e, count, stride=4), :] for e in range(2)
            )
        )
        if parity == 0:
            later = [real * sign, imag * sign]
        else:
            later = [imag * -sign, real * sign]
        row = jnp.concatenate(
            [jnp.concatenate([real, imag], axis=0), jnp.concatenate(later, axis=0)], axis=1
        )
        high = row.astype(jnp.bfloat16)
        low = (row - high.astype(jnp.float32)).astype(jnp.bfloat16)
        both = over_rows(jnp.concatenate([high, low], axis=1), basis_ref[parity, 0])
        more = over_rows(high, basis_ref[parity, 1])
        sums.append(both[: 2 * LANES] + both[2 * LANES :] + more)
    quarter = LON // 4
    for turn in range(4):
        at = turn % 2 * LANES
        even = sums[0][at : at + PART]
        odd = sums[1][at : at + PART]
        cols = slice(turn * quarter, (turn + 1) * quarter)
        out_ref[:, cols] = even + odd if turn < 2 else even - odd


def over_rows(left, right):
    return lax.dot_general(
        left, right, (((0,), (0,)), ((), ())), preferred_element_type=jnp.float32
    )


def synth_call(spectra, signs, waves):
    vm = pltpu.VMEM
    return pl.pallas_call(
        synth_kernel,
        out_shape=jax.ShapeDtypeStruct((PART, LON), jnp.float32),
        in_specs=[pl.BlockSpec(memory_space=vm)] * 3,
        out_specs=pl.BlockSpec(memory_space=vm),
        compiler_params=pltpu.CompilerParams(vmem_limit_bytes=GRANT),
    )(spectra, signs, waves)


def halve_kernel(full_ref, both_ref):
    full = full_ref[...]
    high = full.astype(jnp.bfloat16)
    both_ref[0] = high
    both_ref[1] = (full - high.astype(jnp.float32)).astype(jnp.bfloat16)


def halve_call(full):
    parities, rows, columns = full.shape
    vm = pltpu.VMEM
    return pl.pallas_call(
        halve_kernel,
        grid=(parities,),
        out_shape=vm((parities, 2, rows, columns), jnp.bfloat16),
        in_specs=[pl.BlockSpec((None, rows, columns), lambda p: (p, 0, 0))],
        out_specs=pl.BlockSpec((None, 2, rows, columns), lambda p: (p, 0, 0, 0)),
        compiler_params=pltpu.CompilerParams(vmem_limit_bytes=GRANT),
    )(full)


def basis(pair_wave, slots):
    first = pair_wave.reshape(N_MA, slots).T.reshape(-1)
    other = DEG - 1 - first
    is_even = first % 2 == 0
    waves = jnp.stack([jnp.where(is_even, first, other), jnp.where(is_even, other, first)])
    positions = jnp.arange(QUARTER, dtype=jnp.int32)
    phase = waves[:, :, None] * positions[None, None, :] % LON
    radians = 2.0 * math.pi / LON * phase.astype(jnp.float32)
    weight = jnp.where(waves == 0, 1.0, 2.0).astype(jnp.float32)[:, :, None]
    full = jnp.stack([weight * jnp.cos(radians), -weight * jnp.sin(radians)], axis=1)
    signs = jnp.where(waves % 4 < 2, 1.0, -1.0).astype(jnp.float32)
    return full.reshape(2, -1, QUARTER), signs[:, :, None]


def body(pair_wave, legendre, coefs):
    lat_count = lax.axis_size(LAT)
    lat_place = lax.axis_index(LAT)
    ma_place = lax.axis_index(MA)
    slots, lat_rows = legendre.shape[:2]
    coef_rows = coefs.shape[1]
    sent = pack_call(legendre, coefs, lat_count).reshape(lat_count, -1, 2, LANES)
    got = lax.all_to_all(sent, LAT, split_axis=0, concat_axis=0, tiled=True)
    slot = ma_place * slots + jnp.minimum(lat_place, slots - 1)
    wave = lax.dynamic_slice_in_dim(pair_wave, slot, 1)
    got = pltpu.with_memory_space_constraint(got.reshape(-1, LANES), pltpu.VMEM)
    parts = sums_call(wave, got, lat_count, lat_rows, coef_rows)
    parts = parts.astype(jnp.float16).reshape(lat_count * N_MA, 4, LANES)
    spectra = lax.all_to_all(parts, ALL, split_axis=0, concat_axis=0, tiled=True)
    spectra = spectra[: slots * N_MA].astype(jnp.float32).reshape(-1, LANES)
    full, signs = basis(pair_wave, slots)
    waves = pltpu.with_memory_space_constraint(halve_call(full), pltpu.VMEM)
    spectra = pltpu.with_memory_space_constraint(spectra, pltpu.VMEM)
    return synth_call(spectra, signs, waves)


def solution(mesh):
    split = Mesh(mesh.devices.reshape(8, mesh.shape["lat"] // 8, 4, 2), ALL)
    placed = (P(), P(MA, LAT, None), P(MA, LAT, None))
    return jax.shard_map(
        body, mesh=split, in_specs=placed, out_specs=P(ALL, None), check_vma=False
    )
```

```python
import functools
import math

import jax
import jax.numpy as jnp
from jax import lax
from jax.experimental import pallas as pl
from jax.experimental.pallas import tpu as pltpu
from jax.sharding import Mesh
from jax.sharding import PartitionSpec as P

DEG = 720
LON = 1440
QUARTER = LON // 4
CH = 84
LAT_DEV = 10
N_MA = 8
PART = LAT_DEV * CH // N_MA
LANES = 128
LAT = ("y", "z")
MA = ("x", "core")
ALL = ("y", "z", "x", "core")
TOP = 14
GRANT = 24 * 2**20


def sums_kernel(wave_ref, got_ref, out_ref, *scratch, **sizes):
    @pl.when(wave_ref[0] >= 0)
    def _():
        slot_sums(wave_ref[0], got_ref, out_ref, *scratch, **sizes)

    @pl.when(wave_ref[0] < 0)
    def _():
        out_ref[...] = jnp.zeros_like(out_ref)


def slot_sums(
    wave,
    got_ref,
    out_ref,
    wide_ref,
    weights_ref,
    real_ref,
    imag_ref,
    sums_ref,
    turned_ref,
    *,
    lat_count,
    lat_rows,
    coef_rows,
):
    chunk = got_ref.shape[0] // lat_count
    blocks = DEG // LANES + 1
    depth = lat_count * coef_rows
    wide_ref[...] = got_ref[...].astype(jnp.float32)
    for i in range(lat_rows):
        for b in range(blocks):
            piece = wide_ref[pl.ds(i * blocks + b, lat_count, stride=chunk), :]
            weights_ref[i * lat_count : (i + 1) * lat_count, b * LANES : (b + 1) * LANES] = piece.astype(jnp.bfloat16)
    at = lat_rows * blocks
    tail = 2 * CH - LANES
    split = LANES - CH
    lane = lax.broadcasted_iota(jnp.int32, (lat_count, LANES), 1)
    for k in range(coef_rows):
        main = wide_ref[pl.ds(at + k, lat_count, stride=chunk), :]
        row, place = tail_place(k, lat_rows, coef_rows, blocks, tail)
        rest = wide_ref[pl.ds(row, lat_count, stride=chunk), :]
        moved = pltpu.roll(main, split, 1)
        rest = pltpu.roll(rest, (split - place) % LANES, 1)
        imag = jnp.where(lane < split, moved, rest)
        real_ref[pl.ds(k, lat_count, stride=coef_rows), :] = jnp.where(lane < CH, main, 0.0)
        imag_ref[pl.ds(k, lat_count, stride=coef_rows), :] = jnp.where(lane < CH, imag, 0.0)
    row = lax.broadcasted_iota(jnp.int32, (depth, 2 * LANES), 0)
    inside = row < DEG - wave
    outside = jnp.logical_and(row >= DEG - wave, row <= DEG)
    both = jnp.concatenate([real_ref[...], imag_ref[...]], axis=1)
    is_even = wave % 2 == 0
    first = jnp.where(inside, both, 0.0)
    second = jnp.where(outside, both, 0.0)
    even = jnp.where(is_even, first, second).astype(jnp.bfloat16)
    odd = jnp.where(is_even, second, first).astype(jnp.bfloat16)
    weights = weights_ref[...]
    even = jnp.dot(weights, even, preferred_element_type=jnp.float32)
    odd = jnp.dot(weights, odd, preferred_element_type=jnp.float32)
    sums_ref[:, : 2 * LANES] = even
    sums_ref[:, 2 * LANES :] = odd
    largest = jnp.maximum(jnp.max(jnp.abs(even)), jnp.max(jnp.abs(odd)))
    largest = jnp.maximum(jnp.full((lat_count, LANES), largest, jnp.float32), 1e-30)
    power = jnp.clip(jnp.floor(jnp.log2(largest)), -100.0, 100.0)
    scale = jnp.exp2(TOP - power)
    pitch = turned_ref.shape[0] // lat_count
    for a in range(N_MA):
        i, off = divmod(a * PART, CH)
        for he in range(4):
            cols = slice(he * LANES, (he + 1) * LANES)
            near = sums_ref[i * lat_count : (i + 1) * lat_count, cols]
            far = sums_ref[(i + 1) * lat_count : (i + 2) * lat_count, cols]
            if off:
                near = pltpu.roll(near, LANES - off, 1)
            far = pltpu.roll(far, CH - off, 1)
            value = jnp.where(lane < CH - off, near, far) * scale
            value = jnp.where(lane < PART, value, power)
            turned_ref[pl.ds(a * 4 + he, lat_count, stride=pitch), :] = value
    rows = 4 * N_MA
    for l in range(lat_count):
        out_ref[l * rows : (l + 1) * rows, :] = turned_ref[l * pitch : l * pitch + rows, :]


def sums_call(wave, got, lat_count, lat_rows, coef_rows):
    blocks = DEG // LANES + 1
    vm = pltpu.VMEM
    return pl.pallas_call(
        functools.partial(sums_kernel, lat_count=lat_count, lat_rows=lat_rows, coef_rows=coef_rows),
        out_shape=pltpu.VMEM((lat_count * N_MA * 4, LANES), jnp.float32),
        in_specs=[pl.BlockSpec(memory_space=pltpu.SMEM), pl.BlockSpec(memory_space=vm)],
        out_specs=pl.BlockSpec(memory_space=vm),
        scratch_shapes=[
            vm(got.shape, jnp.float32),
            vm((lat_count * lat_rows, blocks * LANES), jnp.bfloat16),
            vm((lat_count * coef_rows, LANES), jnp.float32),
            vm((lat_count * coef_rows, LANES), jnp.float32),
            vm((lat_count * lat_rows, 4 * LANES), jnp.float32),
            vm((lat_count * (4 * N_MA + 4), LANES), jnp.float32),
        ],
        compiler_params=pltpu.CompilerParams(vmem_limit_bytes=GRANT),
    )(wave, got)


def pack_kernel(legendre_ref, coefs_ref, out_ref, wide_ref):
    lat_rows, slots, degree_rows = legendre_ref.shape
    coef_rows = coefs_ref.shape[0]
    blocks = degree_rows // LANES
    chunk = chunk_rows(lat_rows, coef_rows, blocks)
    tail = 2 * CH - LANES
    top = wide_ref.shape[0]
    wide_ref[top - 16 :, :] = jnp.zeros((16, LANES), jnp.float32)
    for i in range(lat_rows):
        for b in range(blocks):
            piece = legendre_ref[i, :, b * LANES : (b + 1) * LANES].astype(jnp.float32)
            if b == blocks - 1:
                rest = coefs_ref[i, :, LANES:].astype(jnp.float32)
                piece = jnp.concatenate([piece[:, : LANES - tail], rest], axis=1)
            wide_ref[pl.ds(i * blocks + b, slots, stride=chunk), :] = piece
    at = lat_rows * blocks
    for k in range(coef_rows):
        piece = coefs_ref[k, :, :LANES].astype(jnp.float32)
        wide_ref[pl.ds(at + k, slots, stride=chunk), :] = piece
    last = [coefs_ref[k, :, LANES:].astype(jnp.float32) for k in range(lat_rows, coef_rows)]
    last.append(jnp.zeros((slots, LANES - len(last) * tail), jnp.float32))
    last = jnp.concatenate(last, axis=1)
    for t in range(at + coef_rows, chunk):
        wide_ref[pl.ds(t, slots, stride=chunk), :] = last
    out_ref[:top, :] = wide_ref[...].astype(jnp.bfloat16)
    out_ref[top:, :] = jnp.zeros((out_ref.shape[0] - top, LANES), jnp.bfloat16)


def chunk_rows(lat_rows, coef_rows, blocks):
    rows = lat_rows * blocks + coef_rows + 1
    return rows + rows % 2


def tail_place(k, lat_rows, coef_rows, blocks, tail):
    if k < lat_rows:
        return k * blocks + blocks - 1, LANES - tail
    return lat_rows * blocks + coef_rows, (k - lat_rows) * tail


def pack_call(legendre, coefs, lat_count):
    slots, lat_rows, degree_rows = legendre.shape
    coef_rows = coefs.shape[1]
    chunk = chunk_rows(lat_rows, coef_rows, degree_rows // LANES)
    vm = pltpu.VMEM
    return pl.pallas_call(
        pack_kernel,
        out_shape=jax.ShapeDtypeStruct((lat_count * chunk, LANES), jnp.bfloat16),
        in_specs=[pl.BlockSpec(memory_space=vm)] * 2,
        out_specs=pl.BlockSpec(memory_space=vm),
        scratch_shapes=[vm((-(-slots * chunk // 16) * 16, LANES), jnp.float32)],
    )(jnp.transpose(legendre, (1, 0, 2)), jnp.transpose(coefs, (1, 0, 2)))


def synth_kernel(spectra_ref, signs_ref, basis_ref, out_ref):
    count = spectra_ref.shape[0] // 4
    sums = []
    for parity in range(2):
        sign = signs_ref[parity]
        real, imag = (
            row * jnp.exp2(row[:, LANES - 1 :] - TOP)
            for row in (
                spectra_ref[pl.ds(2 * parity + e, count, stride=4), :] for e in range(2)
            )
        )
        if parity == 0:
            later = [real * sign, imag * sign]
        else:
            later = [imag * -sign, real * sign]
        row = jnp.concatenate(
            [jnp.concatenate([real, imag], axis=0), jnp.concatenate(later, axis=0)], axis=1
        )
        high = row.astype(jnp.bfloat16)
        low = (row - high.astype(jnp.float32)).astype(jnp.bfloat16)
        both = over_rows(jnp.concatenate([high, low], axis=1), basis_ref[parity, 0])
        more = over_rows(high, basis_ref[parity, 1])
        sums.append(both[: 2 * LANES] + both[2 * LANES :] + more)
    quarter = LON // 4
    for turn in range(4):
        at = turn % 2 * LANES
        even = sums[0][at : at + PART]
        odd = sums[1][at : at + PART]
        cols = slice(turn * quarter, (turn + 1) * quarter)
        out_ref[:, cols] = even + odd if turn < 2 else even - odd


def over_rows(left, right):
    return lax.dot_general(
        left, right, (((0,), (0,)), ((), ())), preferred_element_type=jnp.float32
    )


def synth_call(spectra, signs, waves):
    vm = pltpu.VMEM
    return pl.pallas_call(
        synth_kernel,
        out_shape=jax.ShapeDtypeStruct((PART, LON), jnp.float32),
        in_specs=[pl.BlockSpec(memory_space=vm)] * 3,
        out_specs=pl.BlockSpec(memory_space=vm),
        compiler_params=pltpu.CompilerParams(vmem_limit_bytes=GRANT),
    )(spectra, signs, waves)


def halve_kernel(full_ref, both_ref):
    full = full_ref[...]
    high = full.astype(jnp.bfloat16)
    both_ref[0] = high
    both_ref[1] = (full - high.astype(jnp.float32)).astype(jnp.bfloat16)


def halve_call(full):
    parities, rows, columns = full.shape
    vm = pltpu.VMEM
    return pl.pallas_call(
        halve_kernel,
        grid=(parities,),
        out_shape=vm((parities, 2, rows, columns), jnp.bfloat16),
        in_specs=[pl.BlockSpec((None, rows, columns), lambda p: (p, 0, 0))],
        out_specs=pl.BlockSpec((None, 2, rows, columns), lambda p: (p, 0, 0, 0)),
        compiler_params=pltpu.CompilerParams(vmem_limit_bytes=GRANT),
    )(full)


def basis(pair_wave, slots):
    first = pair_wave.reshape(N_MA, slots).T.reshape(-1)
    other = DEG - 1 - first
    is_even = first % 2 == 0
    waves = jnp.stack([jnp.where(is_even, first, other), jnp.where(is_even, other, first)])
    positions = jnp.arange(QUARTER, dtype=jnp.int32)
    phase = waves[:, :, None] * positions[None, None, :] % LON
    radians = 2.0 * math.pi / LON * phase.astype(jnp.float32)
    weight = jnp.where(waves == 0, 1.0, 2.0).astype(jnp.float32)[:, :, None]
    full = jnp.stack([weight * jnp.cos(radians), -weight * jnp.sin(radians)], axis=1)
    signs = jnp.where(waves % 4 < 2, 1.0, -1.0).astype(jnp.float32)
    return full.reshape(2, -1, QUARTER), signs[:, :, None]


def body(pair_wave, legendre, coefs):
    lat_count = lax.axis_size(LAT)
    lat_place = lax.axis_index(LAT)
    ma_place = lax.axis_index(MA)
    slots, lat_rows = legendre.shape[:2]
    coef_rows = coefs.shape[1]
    sent = pack_call(legendre, coefs, lat_count).reshape(lat_count, -1, 2, LANES)
    got = lax.all_to_all(sent, LAT, split_axis=0, concat_axis=0, tiled=True)
    slot = ma_place * slots + jnp.minimum(lat_place, slots - 1)
    wave = lax.dynamic_slice_in_dim(pair_wave, slot, 1)
    wave = jnp.where(lat_place < slots, wave, -1)
    got = pltpu.with_memory_space_constraint(got.reshape(-1, LANES), pltpu.VMEM)
    parts = sums_call(wave, got, lat_count, lat_rows, coef_rows)
    parts = parts.astype(jnp.float16).reshape(lat_count * N_MA, 4, LANES)
    spectra = lax.all_to_all(parts, ALL, split_axis=0, concat_axis=0, tiled=True)
    spectra = spectra[: slots * N_MA].astype(jnp.float32).reshape(-1, LANES)
    full, signs = basis(pair_wave, slots)
    waves = pltpu.with_memory_space_constraint(halve_call(full), pltpu.VMEM)
    spectra = pltpu.with_memory_space_constraint(spectra, pltpu.VMEM)
    return synth_call(spectra, signs, waves)


def solution(mesh):
    split = Mesh(mesh.devices.reshape(8, mesh.shape["lat"] // 8, 4, 2), ALL)
    placed = (P(), P(MA, LAT, None), P(MA, LAT, None))
    return jax.shard_map(
        body, mesh=split, in_specs=placed, out_specs=P(ALL, None), check_vma=False
    )
```

```python
import functools
import math

import jax
import jax.numpy as jnp
from jax import lax
from jax.experimental import pallas as pl
from jax.experimental.pallas import tpu as pltpu
from jax.sharding import Mesh
from jax.sharding import PartitionSpec as P

DEG = 720
LON = 1440
QUARTER = LON // 4
CH = 84
LAT_DEV = 10
N_MA = 8
PART = LAT_DEV * CH // N_MA
LANES = 128
LAT = ("y", "z")
MA = ("x", "core")
ALL = ("y", "z", "x", "core")
TOP = 14
GRANT = 24 * 2**20


def sums_kernel(wave_ref, got_ref, out_ref, *scratch, **sizes):
    @pl.when(wave_ref[0] >= 0)
    def _():
        slot_sums(wave_ref[0], got_ref, out_ref, *scratch, **sizes)

    @pl.when(wave_ref[0] < 0)
    def _():
        out_ref[...] = jnp.zeros_like(out_ref)


def slot_sums(
    wave,
    got_ref,
    out_ref,
    wide_ref,
    real_ref,
    imag_ref,
    sums_ref,
    turned_ref,
    *,
    lat_count,
    lat_rows,
    coef_rows,
):
    chunk = got_ref.shape[0] // lat_count
    blocks = DEG // LANES + 1
    depth = lat_count * coef_rows
    wide_ref[...] = got_ref[...].astype(jnp.float32)
    at = lat_rows * blocks
    tail = 2 * CH - LANES
    split = LANES - CH
    lane = lax.broadcasted_iota(jnp.int32, (lat_count, LANES), 1)
    for k in range(coef_rows):
        main = wide_ref[pl.ds(at + k, lat_count, stride=chunk), :]
        row, place = tail_place(k, lat_rows, coef_rows, blocks, tail)
        rest = wide_ref[pl.ds(row, lat_count, stride=chunk), :]
        moved = pltpu.roll(main, split, 1)
        rest = pltpu.roll(rest, (split - place) % LANES, 1)
        imag = jnp.where(lane < split, moved, rest)
        real_ref[pl.ds(k, lat_count, stride=coef_rows), :] = jnp.where(lane < CH, main, 0.0)
        imag_ref[pl.ds(k, lat_count, stride=coef_rows), :] = jnp.where(lane < CH, imag, 0.0)
    row = lax.broadcasted_iota(jnp.int32, (depth, 2 * LANES), 0)
    inside = row < DEG - wave
    outside = jnp.logical_and(row >= DEG - wave, row <= DEG)
    both = jnp.concatenate([real_ref[...], imag_ref[...]], axis=1)
    is_even = wave % 2 == 0
    first = jnp.where(inside, both, 0.0)
    second = jnp.where(outside, both, 0.0)
    even = jnp.where(is_even, first, second).astype(jnp.bfloat16)
    odd = jnp.where(is_even, second, first).astype(jnp.bfloat16)
    right = jnp.concatenate([even, odd], axis=1)
    largest = jnp.zeros((lat_count, 4 * LANES), jnp.float32)
    for i in range(0, lat_rows, 2):
        rows = slice(i * lat_count, (i + 2) * lat_count)
        pieces = [
            jnp.concatenate(
                [
                    wide_ref[pl.ds(n * blocks + b, lat_count, stride=chunk), :].astype(
                        jnp.bfloat16
                    )
                    for b in range(blocks)
                ],
                axis=1,
            )
            for n in (i, i + 1)
        ]
        part = jnp.dot(
            jnp.concatenate(pieces, axis=0), right, preferred_element_type=jnp.float32
        )
        sums_ref[rows, :] = part
        part = jnp.abs(part)
        largest = jnp.maximum(largest, jnp.maximum(part[:lat_count], part[lat_count:]))
    largest = jnp.max(largest)
    largest = jnp.maximum(jnp.full((lat_count, LANES), largest, jnp.float32), 1e-30)
    power = jnp.clip(jnp.floor(jnp.log2(largest)), -100.0, 100.0)
    scale = jnp.exp2(TOP - power)
    pitch = turned_ref.shape[0] // lat_count
    for a in range(N_MA):
        i, off = divmod(a * PART, CH)
        for he in range(4):
            cols = slice(he * LANES, (he + 1) * LANES)
            near = sums_ref[i * lat_count : (i + 1) * lat_count, cols]
            far = sums_ref[(i + 1) * lat_count : (i + 2) * lat_count, cols]
            if off:
                near = pltpu.roll(near, LANES - off, 1)
            far = pltpu.roll(far, CH - off, 1)
            value = jnp.where(lane < CH - off, near, far) * scale
            value = jnp.where(lane < PART, value, power)
            turned_ref[pl.ds(a * 4 + he, lat_count, stride=pitch), :] = value
    rows = 4 * N_MA
    for l in range(lat_count):
        out_ref[l * rows : (l + 1) * rows, :] = turned_ref[l * pitch : l * pitch + rows, :]


def sums_call(wave, got, lat_count, lat_rows, coef_rows):
    blocks = DEG // LANES + 1
    vm = pltpu.VMEM
    return pl.pallas_call(
        functools.partial(sums_kernel, lat_count=lat_count, lat_rows=lat_rows, coef_rows=coef_rows),
        out_shape=pltpu.VMEM((lat_count * N_MA * 4, LANES), jnp.float32),
        in_specs=[pl.BlockSpec(memory_space=pltpu.SMEM), pl.BlockSpec(memory_space=vm)],
        out_specs=pl.BlockSpec(memory_space=vm),
        scratch_shapes=[
            vm(got.shape, jnp.float32),
            vm((lat_count * coef_rows, LANES), jnp.float32),
            vm((lat_count * coef_rows, LANES), jnp.float32),
            vm((lat_count * lat_rows, 4 * LANES), jnp.float32),
            vm((lat_count * (4 * N_MA + 4), LANES), jnp.float32),
        ],
        compiler_params=pltpu.CompilerParams(vmem_limit_bytes=GRANT),
    )(wave, got)


def pack_kernel(legendre_ref, coefs_ref, out_ref, wide_ref):
    lat_rows, slots, degree_rows = legendre_ref.shape
    coef_rows = coefs_ref.shape[0]
    blocks = degree_rows // LANES
    chunk = chunk_rows(lat_rows, coef_rows, blocks)
    tail = 2 * CH - LANES
    top = wide_ref.shape[0]
    wide_ref[top - 16 :, :] = jnp.zeros((16, LANES), jnp.float32)
    for i in range(lat_rows):
        for b in range(blocks):
            piece = legendre_ref[i, :, b * LANES : (b + 1) * LANES].astype(jnp.float32)
            if b == blocks - 1:
                rest = coefs_ref[i, :, LANES:].astype(jnp.float32)
                piece = jnp.concatenate([piece[:, : LANES - tail], rest], axis=1)
            wide_ref[pl.ds(i * blocks + b, slots, stride=chunk), :] = piece
    at = lat_rows * blocks
    for k in range(coef_rows):
        piece = coefs_ref[k, :, :LANES].astype(jnp.float32)
        wide_ref[pl.ds(at + k, slots, stride=chunk), :] = piece
    last = [coefs_ref[k, :, LANES:].astype(jnp.float32) for k in range(lat_rows, coef_rows)]
    last.append(jnp.zeros((slots, LANES - len(last) * tail), jnp.float32))
    last = jnp.concatenate(last, axis=1)
    for t in range(at + coef_rows, chunk):
        wide_ref[pl.ds(t, slots, stride=chunk), :] = last
    out_ref[:top, :] = wide_ref[...].astype(jnp.bfloat16)
    out_ref[top:, :] = jnp.zeros((out_ref.shape[0] - top, LANES), jnp.bfloat16)


def chunk_rows(lat_rows, coef_rows, blocks):
    rows = lat_rows * blocks + coef_rows + 1
    return rows + rows % 2


def tail_place(k, lat_rows, coef_rows, blocks, tail):
    if k < lat_rows:
        return k * blocks + blocks - 1, LANES - tail
    return lat_rows * blocks + coef_rows, (k - lat_rows) * tail


def pack_call(legendre, coefs, lat_count):
    slots, lat_rows, degree_rows = legendre.shape
    coef_rows = coefs.shape[1]
    chunk = chunk_rows(lat_rows, coef_rows, degree_rows // LANES)
    vm = pltpu.VMEM
    return pl.pallas_call(
        pack_kernel,
        out_shape=jax.ShapeDtypeStruct((lat_count * chunk, LANES), jnp.bfloat16),
        in_specs=[pl.BlockSpec(memory_space=vm)] * 2,
        out_specs=pl.BlockSpec(memory_space=vm),
        scratch_shapes=[vm((-(-slots * chunk // 16) * 16, LANES), jnp.float32)],
    )(jnp.transpose(legendre, (1, 0, 2)), jnp.transpose(coefs, (1, 0, 2)))


def synth_kernel(spectra_ref, signs_ref, basis_ref, out_ref):
    count = spectra_ref.shape[0] // 4
    sums = []
    for parity in range(2):
        sign = signs_ref[parity]
        real, imag = (
            row * jnp.exp2(row[:, LANES - 1 :] - TOP)
            for row in (
                spectra_ref[pl.ds(2 * parity + e, count, stride=4), :] for e in range(2)
            )
        )
        if parity == 0:
            later = [real * sign, imag * sign]
        else:
            later = [imag * -sign, real * sign]
        row = jnp.concatenate(
            [jnp.concatenate([real, imag], axis=0), jnp.concatenate(later, axis=0)], axis=1
        )
        high = row.astype(jnp.bfloat16)
        low = (row - high.astype(jnp.float32)).astype(jnp.bfloat16)
        both = over_rows(jnp.concatenate([high, low], axis=1), basis_ref[parity, 0])
        more = over_rows(high, basis_ref[parity, 1])
        sums.append(both[: 2 * LANES] + both[2 * LANES :] + more)
    quarter = LON // 4
    for turn in range(4):
        at = turn % 2 * LANES
        even = sums[0][at : at + PART]
        odd = sums[1][at : at + PART]
        cols = slice(turn * quarter, (turn + 1) * quarter)
        out_ref[:, cols] = even + odd if turn < 2 else even - odd


def over_rows(left, right):
    return lax.dot_general(
        left, right, (((0,), (0,)), ((), ())), preferred_element_type=jnp.float32
    )


def synth_call(spectra, signs, waves):
    vm = pltpu.VMEM
    return pl.pallas_call(
        synth_kernel,
        out_shape=jax.ShapeDtypeStruct((PART, LON), jnp.float32),
        in_specs=[pl.BlockSpec(memory_space=vm)] * 3,
        out_specs=pl.BlockSpec(memory_space=vm),
        compiler_params=pltpu.CompilerParams(vmem_limit_bytes=GRANT),
    )(spectra, signs, waves)


def halve_kernel(full_ref, both_ref):
    full = full_ref[...]
    high = full.astype(jnp.bfloat16)
    both_ref[0] = high
    both_ref[1] = (full - high.astype(jnp.float32)).astype(jnp.bfloat16)


def halve_call(full):
    parities, rows, columns = full.shape
    vm = pltpu.VMEM
    return pl.pallas_call(
        halve_kernel,
        grid=(parities,),
        out_shape=vm((parities, 2, rows, columns), jnp.bfloat16),
        in_specs=[pl.BlockSpec((None, rows, columns), lambda p: (p, 0, 0))],
        out_specs=pl.BlockSpec((None, 2, rows, columns), lambda p: (p, 0, 0, 0)),
        compiler_params=pltpu.CompilerParams(vmem_limit_bytes=GRANT),
    )(full)


def basis(pair_wave, slots):
    first = pair_wave.reshape(N_MA, slots).T.reshape(-1)
    other = DEG - 1 - first
    is_even = first % 2 == 0
    waves = jnp.stack([jnp.where(is_even, first, other), jnp.where(is_even, other, first)])
    positions = jnp.arange(QUARTER, dtype=jnp.int32)
    phase = waves[:, :, None] * positions[None, None, :] % LON
    radians = 2.0 * math.pi / LON * phase.astype(jnp.float32)
    weight = jnp.where(waves == 0, 1.0, 2.0).astype(jnp.float32)[:, :, None]
    full = jnp.stack([weight * jnp.cos(radians), -weight * jnp.sin(radians)], axis=1)
    signs = jnp.where(waves % 4 < 2, 1.0, -1.0).astype(jnp.float32)
    return full.reshape(2, -1, QUARTER), signs[:, :, None]


def body(pair_wave, legendre, coefs):
    lat_count = lax.axis_size(LAT)
    lat_place = lax.axis_index(LAT)
    ma_place = lax.axis_index(MA)
    slots, lat_rows = legendre.shape[:2]
    coef_rows = coefs.shape[1]
    sent = pack_call(legendre, coefs, lat_count).reshape(lat_count, -1, 2, LANES)
    got = lax.all_to_all(sent, LAT, split_axis=0, concat_axis=0, tiled=True)
    slot = ma_place * slots + jnp.minimum(lat_place, slots - 1)
    wave = lax.dynamic_slice_in_dim(pair_wave, slot, 1)
    wave = jnp.where(lat_place < slots, wave, -1)
    got = pltpu.with_memory_space_constraint(got.reshape(-1, LANES), pltpu.VMEM)
    parts = sums_call(wave, got, lat_count, lat_rows, coef_rows)
    parts = parts.astype(jnp.float16).reshape(lat_count * N_MA, 4, LANES)
    spectra = lax.all_to_all(parts, ALL, split_axis=0, concat_axis=0, tiled=True)
    spectra = spectra[: slots * N_MA].astype(jnp.float32).reshape(-1, LANES)
    full, signs = basis(pair_wave, slots)
    waves = pltpu.with_memory_space_constraint(halve_call(full), pltpu.VMEM)
    spectra = pltpu.with_memory_space_constraint(spectra, pltpu.VMEM)
    return synth_call(spectra, signs, waves)


def solution(mesh):
    split = Mesh(mesh.devices.reshape(8, mesh.shape["lat"] // 8, 4, 2), ALL)
    placed = (P(), P(MA, LAT, None), P(MA, LAT, None))
    return jax.shard_map(
        body, mesh=split, in_specs=placed, out_specs=P(ALL, None), check_vma=False
    )
```

```python
import functools
import math

import jax
import jax.numpy as jnp
from jax import lax
from jax.experimental import pallas as pl
from jax.experimental.pallas import tpu as pltpu
from jax.sharding import Mesh
from jax.sharding import PartitionSpec as P

DEG = 720
LON = 1440
QUARTER = LON // 4
CH = 84
LAT_DEV = 10
N_MA = 8
PART = LAT_DEV * CH // N_MA
LANES = 128
LAT = ("y", "z")
MA = ("x", "core")
ALL = ("y", "z", "x", "core")
TOP = 14
GRANT = 24 * 2**20


def sums_kernel(wave_ref, got_ref, out_ref, *scratch, **sizes):
    @pl.when(wave_ref[0] >= 0)
    def _():
        slot_sums(wave_ref[0], got_ref, out_ref, *scratch, **sizes)

    @pl.when(wave_ref[0] < 0)
    def _():
        out_ref[...] = jnp.zeros_like(out_ref)


def slot_sums(
    wave,
    got_ref,
    out_ref,
    wide_ref,
    real_ref,
    imag_ref,
    sums_ref,
    turned_ref,
    *,
    lat_count,
    lat_rows,
    coef_rows,
):
    chunk = got_ref.shape[0] // lat_count
    blocks = DEG // LANES + 1
    depth = lat_count * coef_rows
    wide_ref[...] = got_ref[...].astype(jnp.float32)
    at = lat_rows * blocks
    tail = 2 * CH - LANES
    split = LANES - CH
    lane = lax.broadcasted_iota(jnp.int32, (lat_count, LANES), 1)
    for k in range(coef_rows):
        main = wide_ref[pl.ds(at + k, lat_count, stride=chunk), :]
        row, place = tail_place(k, lat_rows, coef_rows, blocks, tail)
        rest = wide_ref[pl.ds(row, lat_count, stride=chunk), :]
        moved = pltpu.roll(main, split, 1)
        rest = pltpu.roll(rest, (split - place) % LANES, 1)
        imag = jnp.where(lane < split, moved, rest)
        real_ref[pl.ds(k, lat_count, stride=coef_rows), :] = jnp.where(lane < CH, main, 0.0)
        imag_ref[pl.ds(k, lat_count, stride=coef_rows), :] = jnp.where(lane < CH, imag, 0.0)
    row = lax.broadcasted_iota(jnp.int32, (depth, 2 * LANES), 0)
    inside = row < DEG - wave
    outside = jnp.logical_and(row >= DEG - wave, row <= DEG)
    both = jnp.concatenate([real_ref[...], imag_ref[...]], axis=1)
    is_even = wave % 2 == 0
    first = jnp.where(inside, both, 0.0)
    second = jnp.where(outside, both, 0.0)
    even = jnp.where(is_even, first, second).astype(jnp.bfloat16)
    odd = jnp.where(is_even, second, first).astype(jnp.bfloat16)
    right = jnp.concatenate([even, odd], axis=1)
    largest = jnp.zeros((lat_count, 4 * LANES), jnp.float32)
    for i in range(0, lat_rows, 2):
        rows = slice(i * lat_count, (i + 2) * lat_count)
        pieces = [
            jnp.concatenate(
                [
                    wide_ref[pl.ds(n * blocks + b, lat_count, stride=chunk), :].astype(
                        jnp.bfloat16
                    )
                    for b in range(blocks)
                ],
                axis=1,
            )
            for n in (i, i + 1)
        ]
        part = jnp.dot(
            jnp.concatenate(pieces, axis=0), right, preferred_element_type=jnp.float32
        )
        sums_ref[rows, :] = part
        part = jnp.abs(part)
        largest = jnp.maximum(largest, jnp.maximum(part[:lat_count], part[lat_count:]))
    largest = jnp.max(largest)
    largest = jnp.maximum(jnp.full((lat_count, LANES), largest, jnp.float32), 1e-30)
    power = jnp.clip(jnp.floor(jnp.log2(largest)), -100.0, 100.0)
    scale = jnp.exp2(TOP - power)
    pitch = turned_ref.shape[0] // lat_count
    for a in range(N_MA):
        i, off = divmod(a * PART, CH)
        for he in range(4):
            cols = slice(he * LANES, (he + 1) * LANES)
            near = sums_ref[i * lat_count : (i + 1) * lat_count, cols]
            far = sums_ref[(i + 1) * lat_count : (i + 2) * lat_count, cols]
            if off:
                near = pltpu.roll(near, LANES - off, 1)
            far = pltpu.roll(far, CH - off, 1)
            value = jnp.where(lane < CH - off, near, far) * scale
            value = jnp.where(lane < PART, value, power)
            turned_ref[pl.ds(a * 4 + he, lat_count, stride=pitch), :] = value
    rows = 4 * N_MA
    for l in range(lat_count):
        out_ref[l * rows : (l + 1) * rows, :] = turned_ref[l * pitch : l * pitch + rows, :]


def sums_call(wave, got, lat_count, lat_rows, coef_rows):
    blocks = DEG // LANES + 1
    vm = pltpu.VMEM
    return pl.pallas_call(
        functools.partial(sums_kernel, lat_count=lat_count, lat_rows=lat_rows, coef_rows=coef_rows),
        out_shape=pltpu.VMEM((lat_count * N_MA * 4, LANES), jnp.float32),
        in_specs=[pl.BlockSpec(memory_space=pltpu.SMEM), pl.BlockSpec(memory_space=vm)],
        out_specs=pl.BlockSpec(memory_space=vm),
        scratch_shapes=[
            vm(got.shape, jnp.float32),
            vm((lat_count * coef_rows, LANES), jnp.float32),
            vm((lat_count * coef_rows, LANES), jnp.float32),
            vm((lat_count * lat_rows, 4 * LANES), jnp.float32),
            vm((lat_count * (4 * N_MA + 4), LANES), jnp.float32),
        ],
        compiler_params=pltpu.CompilerParams(vmem_limit_bytes=GRANT),
    )(wave, got)


def pack_kernel(legendre_ref, coefs_ref, out_ref, wide_ref):
    lat_rows, slots, degree_rows = legendre_ref.shape
    coef_rows = coefs_ref.shape[0]
    blocks = degree_rows // LANES
    chunk = chunk_rows(lat_rows, coef_rows, blocks)
    tail = 2 * CH - LANES
    top = -(-slots * chunk // 16) * 16
    wide_ref[top - 16 : top, :] = jnp.zeros((16, LANES), jnp.float32)
    for i in range(lat_rows):
        for b in range(blocks):
            piece = legendre_ref[i, :, b * LANES : (b + 1) * LANES].astype(jnp.float32)
            if b == blocks - 1:
                rest = coefs_ref[i, :, LANES:].astype(jnp.float32)
                piece = jnp.concatenate([piece[:, : LANES - tail], rest], axis=1)
            wide_ref[pl.ds(i * blocks + b, slots, stride=chunk), :] = piece
    at = lat_rows * blocks
    for k in range(coef_rows):
        piece = coefs_ref[k, :, :LANES].astype(jnp.float32)
        wide_ref[pl.ds(at + k, slots, stride=chunk), :] = piece
    last = [coefs_ref[k, :, LANES:].astype(jnp.float32) for k in range(lat_rows, coef_rows)]
    last.append(jnp.zeros((slots, LANES - len(last) * tail), jnp.float32))
    last = jnp.concatenate(last, axis=1)
    for t in range(at + coef_rows, chunk):
        wide_ref[pl.ds(t, slots, stride=chunk), :] = last
    out_ref[:top, :] = wide_ref[:top, :].astype(jnp.bfloat16)
    out_ref[top:, :] = jnp.zeros((out_ref.shape[0] - top, LANES), jnp.bfloat16)


def chunk_rows(lat_rows, coef_rows, blocks):
    rows = lat_rows * blocks + coef_rows + 1
    return rows + rows % 2


def tail_place(k, lat_rows, coef_rows, blocks, tail):
    if k < lat_rows:
        return k * blocks + blocks - 1, LANES - tail
    return lat_rows * blocks + coef_rows, (k - lat_rows) * tail


def pack_call(legendre, coefs, lat_count):
    slots, lat_rows, degree_rows = legendre.shape
    coef_rows = coefs.shape[1]
    chunk = chunk_rows(lat_rows, coef_rows, degree_rows // LANES)
    vm = pltpu.VMEM
    return pl.pallas_call(
        pack_kernel,
        out_shape=jax.ShapeDtypeStruct((lat_count * chunk, LANES), jnp.bfloat16),
        in_specs=[pl.BlockSpec(memory_space=vm)] * 2,
        out_specs=pl.BlockSpec(memory_space=vm),
        scratch_shapes=[vm((-(-slots // 8) * 8 * chunk, LANES), jnp.float32)],
    )(jnp.transpose(legendre, (1, 0, 2)), jnp.transpose(coefs, (1, 0, 2)))


def synth_kernel(spectra_ref, signs_ref, basis_ref, out_ref):
    count = spectra_ref.shape[0] // 4
    sums = []
    for parity in range(2):
        sign = signs_ref[parity]
        real, imag = (
            row * jnp.exp2(row[:, LANES - 1 :] - TOP)
            for row in (
                spectra_ref[pl.ds(2 * parity + e, count, stride=4), :] for e in range(2)
            )
        )
        if parity == 0:
            later = [real * sign, imag * sign]
        else:
            later = [imag * -sign, real * sign]
        row = jnp.concatenate(
            [jnp.concatenate([real, imag], axis=0), jnp.concatenate(later, axis=0)], axis=1
        )
        high = row.astype(jnp.bfloat16)
        low = (row - high.astype(jnp.float32)).astype(jnp.bfloat16)
        both = over_rows(jnp.concatenate([high, low], axis=1), basis_ref[parity, 0])
        more = over_rows(high, basis_ref[parity, 1])
        sums.append(both[: 2 * LANES] + both[2 * LANES :] + more)
    quarter = LON // 4
    for turn in range(4):
        at = turn % 2 * LANES
        even = sums[0][at : at + PART]
        odd = sums[1][at : at + PART]
        cols = slice(turn * quarter, (turn + 1) * quarter)
        out_ref[:, cols] = even + odd if turn < 2 else even - odd


def over_rows(left, right):
    return lax.dot_general(
        left, right, (((0,), (0,)), ((), ())), preferred_element_type=jnp.float32
    )


def synth_call(spectra, signs, waves):
    vm = pltpu.VMEM
    return pl.pallas_call(
        synth_kernel,
        out_shape=jax.ShapeDtypeStruct((PART, LON), jnp.float32),
        in_specs=[pl.BlockSpec(memory_space=vm)] * 3,
        out_specs=pl.BlockSpec(memory_space=vm),
        compiler_params=pltpu.CompilerParams(vmem_limit_bytes=GRANT),
    )(spectra, signs, waves)


def halve_kernel(full_ref, both_ref):
    full = full_ref[...]
    high = full.astype(jnp.bfloat16)
    both_ref[0] = high
    both_ref[1] = (full - high.astype(jnp.float32)).astype(jnp.bfloat16)


def halve_call(full):
    parities, rows, columns = full.shape
    vm = pltpu.VMEM
    return pl.pallas_call(
        halve_kernel,
        grid=(parities,),
        out_shape=vm((parities, 2, rows, columns), jnp.bfloat16),
        in_specs=[pl.BlockSpec((None, rows, columns), lambda p: (p, 0, 0))],
        out_specs=pl.BlockSpec((None, 2, rows, columns), lambda p: (p, 0, 0, 0)),
        compiler_params=pltpu.CompilerParams(vmem_limit_bytes=GRANT),
    )(full)


def basis(pair_wave, slots):
    first = pair_wave.reshape(N_MA, slots).T.reshape(-1)
    other = DEG - 1 - first
    is_even = first % 2 == 0
    waves = jnp.stack([jnp.where(is_even, first, other), jnp.where(is_even, other, first)])
    positions = jnp.arange(QUARTER, dtype=jnp.int32)
    phase = waves[:, :, None] * positions[None, None, :] % LON
    radians = 2.0 * math.pi / LON * phase.astype(jnp.float32)
    weight = jnp.where(waves == 0, 1.0, 2.0).astype(jnp.float32)[:, :, None]
    full = jnp.stack([weight * jnp.cos(radians), -weight * jnp.sin(radians)], axis=1)
    signs = jnp.where(waves % 4 < 2, 1.0, -1.0).astype(jnp.float32)
    return full.reshape(2, -1, QUARTER), signs[:, :, None]


def body(pair_wave, legendre, coefs):
    lat_count = lax.axis_size(LAT)
    lat_place = lax.axis_index(LAT)
    ma_place = lax.axis_index(MA)
    slots, lat_rows = legendre.shape[:2]
    coef_rows = coefs.shape[1]
    sent = pack_call(legendre, coefs, lat_count).reshape(lat_count, -1, 2, LANES)
    got = lax.all_to_all(sent, LAT, split_axis=0, concat_axis=0, tiled=True)
    slot = ma_place * slots + jnp.minimum(lat_place, slots - 1)
    wave = lax.dynamic_slice_in_dim(pair_wave, slot, 1)
    wave = jnp.where(lat_place < slots, wave, -1)
    got = pltpu.with_memory_space_constraint(got.reshape(-1, LANES), pltpu.VMEM)
    parts = sums_call(wave, got, lat_count, lat_rows, coef_rows)
    parts = parts.astype(jnp.float16).reshape(lat_count * N_MA, 4, LANES)
    spectra = lax.all_to_all(parts, ALL, split_axis=0, concat_axis=0, tiled=True)
    spectra = spectra[: slots * N_MA].astype(jnp.float32).reshape(-1, LANES)
    full, signs = basis(pair_wave, slots)
    waves = pltpu.with_memory_space_constraint(halve_call(full), pltpu.VMEM)
    spectra = pltpu.with_memory_space_constraint(spectra, pltpu.VMEM)
    return synth_call(spectra, signs, waves)


def solution(mesh):
    split = Mesh(mesh.devices.reshape(8, mesh.shape["lat"] // 8, 4, 2), ALL)
    placed = (P(), P(MA, LAT, None), P(MA, LAT, None))
    return jax.shard_map(
        body, mesh=split, in_specs=placed, out_specs=P(ALL, None), check_vma=False
    )
```
